256 devices in a mesh: leaf: 128 (over x, y, z), sub: 2 (over core).
Axes of the slice: x: 4, y: 4, z: 8, core: 2. Of those that a mesh axis runs over, the one named last changes fastest.
Arguments:
- points: float32 [2, 2097152], P(None, ('leaf', 'sub')), may hold values from 0 to 1
- right_sides: float32 [32, 2097152], P(None, ('leaf', 'sub')), may hold values from -0.6 to 0.6
- leaf_order: int32 [16384], P(('leaf', 'sub')), may hold values from 0 to 63, as said below
- leaf_basis: float32 [16384, 32, 128], P(('leaf', 'sub')), may hold values from -0.5 to 0.5
- transfer_low: float32 [4096, 32, 128], P(('leaf', 'sub')), may hold values from -0.5 to 0.5
- transfer_top: float32 [4096, 32, 32], P(('leaf', 'sub')), may hold values from -0.1875 to 0.1875
- proxy_low: float32 [4096, 2, 32], P(('leaf', 'sub')), may hold values from 0 to 1
- proxy_top: float32 [128, 2, 32], replicated, may hold values from 0 to 1
- near_lists: int32 [16384, 9], P(('leaf', 'sub')), may hold values from 0 to 16383, as said below
- far_lists: int32 [4096, 27], P(('leaf', 'sub')), may hold values from 0 to 4095, as said below
- top_lists: int32 [128, 27], P('leaf'), may hold values from 0 to 127
- subtree_map: int32 [128], replicated, may hold values from 0 to 127, each once
Outputs:
- product: float32 [32, 2097152], P(None, ('leaf', 'sub'))
The draws below stay inside these ranges and needn't reach their ends.
Inputs may be any that keep to these rules, and one draw needn't show every extreme that they name: `leaf_order`: each device's block of 64 entries is a permutation of 0 to 63. `near_lists`: entries are global leaf numbers; leaf s lies on device s // 64, devices numbered leaf index times the size of sub plus sub index and laid out in rows of 16. Of the entries of one device's leaves exactly 256 lie on other devices, all on the devices beside it in its row or in its column (number one less or one more in the same row of 16, or 16 less or 16 more), at most 128 on any one of them, and for every device some such neighbour holds exactly 128. `far_lists`: entries are global cluster numbers; cluster s lies on device s // 16, and the sources of a device's clusters lie on that device or on the devices numbered one less or one more.
All inputs are finite; a program needn't handle non-finite values.
Results may differ from the reference program's by a relative error of at most 0.00017.
Values sent between devices are 32-bit elements; how exact they have to be, the bound alone decides.
No kernel may reach another device: no remote copies, remote signals or barrier semaphores. Data moves between devices by JAX's collectives and lax.ppermute only.
A program may use at most 128 MiB of HBM per device.

```python
import jax
import jax.numpy as jnp
from jax import lax

LEAF = 128
RANK = 32
RHS = 32
LPD = 64
NEAR = 9
FAR1 = 27
FAR2 = 27
CAP = 128
NPTS = 2097152
NLEAVES = 16384
NC_DEV = 16
NC1 = 4096
SUBTREES = 128
REMOTE = 256


def draw_leaf_order(key, part):
    device_count = NLEAVES // LPD
    device_keys = jax.random.split(jax.random.fold_in(key, 3), device_count)
    blocks = jax.vmap(lambda single: jax.random.permutation(single, LPD))(device_keys)
    return blocks.reshape(-1).astype(jnp.int32)


def near_block(single, device):
    device_count = NLEAVES // LPD
    row_count = device_count // 16
    task_count = LPD * NEAR
    first_key, second, third, fourth = jax.random.split(single, 4)
    column = device % 16
    row_number = device // 16
    offsets = jnp.array([-16, -1, 1, 16], dtype=jnp.int32)
    valid = jnp.stack([row_number > 0, column > 0, column < 15, row_number < row_count - 1]).astype(jnp.int32)
    forced = jnp.argmax(valid).astype(jnp.int32)
    slot_ids = jnp.arange(4 * CAP, dtype=jnp.int32)
    neighbour = slot_ids // CAP
    scores = jax.random.permutation(first_key, 4 * CAP).astype(jnp.int32)
    scores = jnp.where(neighbour == forced, -1, scores)
    scores = jnp.where(valid[neighbour] == 0, 8 * CAP, scores)
    chosen = jnp.argsort(scores, stable=True)[:REMOTE].astype(jnp.int32)
    owners = device + offsets[chosen // CAP]
    remote = owners * LPD + jax.random.randint(second, (REMOTE,), 0, LPD)
    local_ids = device * LPD + jax.random.randint(third, (task_count - REMOTE,), 0, LPD)
    joined = jnp.concatenate([remote, local_ids]).astype(jnp.int32)
    return joined[jax.random.permutation(fourth, task_count)].reshape(LPD, NEAR)


def draw_near_lists(key, part):
    device_count = NLEAVES // LPD
    device_keys = jax.random.split(jax.random.fold_in(key, 7), device_count)
    blocks = jax.vmap(near_block)(device_keys, jnp.arange(device_count, dtype=jnp.int32))
    return blocks.reshape(NLEAVES, NEAR).astype(jnp.int32)


def draw_far_lists(key, part):
    first_key, second = jax.random.split(jax.random.fold_in(key, 11))
    device = jnp.arange(NC1, dtype=jnp.int32)[:, None] // NC_DEV
    offset = jax.random.randint(first_key, (NC1, FAR1), -1, 2)
    chosen = jnp.clip(device + offset, 0, NC1 // NC_DEV - 1)
    return (chosen * NC_DEV + jax.random.randint(second, (NC1, FAR1), 0, NC_DEV)).astype(jnp.int32)


def plant(values, stream_key, smallest, largest):
    extent = values.shape
    place = [jax.random.randint(jax.random.fold_in(stream_key, axis), (), 0, extent[axis]) for axis in range(len(extent))]
    values = values.at[tuple(place)].set(smallest)
    longest = extent.index(max(extent))
    place[longest] = (place[longest] + 1) % extent[longest]
    return values.at[tuple(place)].set(largest)


def shard_levels(own_key, shape, cuts, least, top_value):
    gain = 1.0
    for position, parts in cuts:
        draws = jax.random.uniform(jax.random.fold_in(jax.random.fold_in(own_key, 6), position), (parts,), jnp.float32, least / len(cuts), top_value / len(cuts))
        gain = gain * jnp.repeat(jnp.exp(draws), shape[position] // parts).reshape((-1,) + (1,) * (len(shape) - 1 - position))
    return gain


def noise(rng, shape, deviation, limit, cuts=(), held_as=jnp.bfloat16):
    values = jax.random.normal(rng, shape, jnp.float32) * deviation
    if len(cuts) > 0:
        values = shard_levels(rng, shape, cuts, -0.22, 0.18) * values
    return jnp.clip(values, min=-limit, max=limit).astype(held_as)


def setup_inputs(seed: int = 0) -> dict:
    splits = jax.random.split(jax.random.key(seed), 13)
    return {
        "points": jnp.clip(1.0 * jax.random.uniform(splits[0], (2, NPTS), jnp.float32) ** shard_levels(splits[0], (2, NPTS), ((1, 256),), -0.2, 0.2), 0.0, 1.0),
        "right_sides": noise(splits[1], (RHS, NPTS), 0.1, 0.6, ((1, 256),), jnp.float32),
        "leaf_order": draw_leaf_order(jax.random.fold_in(splits[12], 71), 0),
        "leaf_basis": noise(splits[3], (NLEAVES, RANK, LEAF), LEAF ** -0.5, 0.5, ((0, 256),), jnp.float32),
        "transfer_low": noise(splits[4], (NC1, RANK, 4 * RANK), (4 * RANK) ** -0.5, 0.5, ((0, 256),), jnp.float32),
        "transfer_top": noise(splits[5], (NC1, RANK, RANK), (2 * RANK * NC_DEV) ** -0.5, 0.1875, ((0, 256),), jnp.float32),
        "proxy_low": jnp.clip(1.0 * jax.random.uniform(splits[6], (NC1, 2, RANK), jnp.float32) ** shard_levels(splits[6], (NC1, 2, RANK), ((0, 256),), -0.2, 0.2), 0.0, 1.0),
        "proxy_top": jnp.clip(jax.random.uniform(splits[7], (SUBTREES, 2, RANK), jnp.float32, 0.0, 1.0), 0.0, 1.0),
        "near_lists": draw_near_lists(jax.random.fold_in(splits[12], 71), 0),
        "far_lists": draw_far_lists(jax.random.fold_in(splits[12], 71), 0),
        "top_lists": plant(jax.random.randint(splits[10], (SUBTREES, FAR2), 0, SUBTREES), jax.random.fold_in(splits[10], 1), 0, SUBTREES - 1).astype(jnp.int32),
        "subtree_map": jax.random.permutation(splits[11], SUBTREES).astype(jnp.int32),
    }


length_scale = 0.25
highest = lax.Precision.HIGHEST

def kernel_block(first_points, second):
    delta_x = first_points[..., 0, :, None] - second[..., 0, None, :]
    delta_y = first_points[..., 1, :, None] - second[..., 1, None, :]
    return jnp.exp(-jnp.sqrt(delta_x * delta_x + delta_y * delta_y) / length_scale)

def reference(points, right_sides, leaf_order, leaf_basis, transfer_low, transfer_top, proxy_low, proxy_top, near_lists, far_lists, top_lists, subtree_map):
    leaf_ids = jnp.arange(NLEAVES, dtype=jnp.int32)
    source_block = (leaf_order + leaf_ids // LPD * LPD).astype(jnp.int32)
    leaf_xy = points.reshape(2, NLEAVES, LEAF).transpose(1, 0, 2)[source_block]
    leaf_values = right_sides.reshape(RHS, NLEAVES, LEAF).transpose(1, 0, 2)[source_block]
    coef_leaf = jnp.einsum('bql,brl->bqr', leaf_values, leaf_basis, precision=highest)
    stacked = coef_leaf.reshape(NC1, 4, RHS, RANK).transpose(0, 2, 1, 3).reshape(NC1, RHS, 4 * RANK)
    coef_low = jnp.einsum('cqk,crk->cqr', stacked, transfer_low, precision=highest)
    coef_top = jnp.einsum('cqr,crs->cqs', coef_low, transfer_top, precision=highest)
    coef_top = coef_top.reshape(SUBTREES, NC1 // SUBTREES, RHS, RANK).sum(axis=1)
    source_chips = subtree_map[top_lists]
    coupling_top = kernel_block(proxy_top[:, None], proxy_top[source_chips])
    down_top = jnp.einsum('akqs,akts->aqt', coef_top[source_chips], coupling_top, precision=highest)

    def cluster_down(cluster_id):
        source_ids = far_lists[cluster_id]
        coupling = kernel_block(proxy_low[cluster_id], proxy_low[source_ids])
        return jnp.einsum('kqs,kts->qt', coef_low[source_ids], coupling, precision=highest)
    down_low = lax.map(cluster_down, jnp.arange(NC1, dtype=jnp.int32), batch_size=256)
    chip_of = jnp.arange(NC1, dtype=jnp.int32) // (NC1 // SUBTREES)
    down_low = down_low + jnp.einsum('cqs,crs->cqr', down_top[chip_of], transfer_top, precision=highest)
    down_stack = jnp.einsum('cqr,crk->cqk', down_low, transfer_low, precision=highest)
    down_leaf = down_stack.reshape(NC1, RHS, 4, RANK).transpose(0, 2, 1, 3).reshape(NLEAVES, RHS, RANK)
    far_part = jnp.einsum('bqr,brl->bql', down_leaf, leaf_basis, precision=highest)

    def leaf_near(leaf_id):
        source_ids = near_lists[leaf_id]
        kernel = kernel_block(leaf_xy[leaf_id], leaf_xy[source_ids])
        return jnp.einsum('kqj,kij->qi', leaf_values[source_ids], kernel, precision=highest)
    near_part = lax.map(leaf_near, leaf_ids, batch_size=16)
    leaf_result = far_part + near_part
    placed = jnp.zeros_like(leaf_result).at[source_block].set(leaf_result)
    return placed.transpose(1, 0, 2).reshape(RHS, NPTS)
```

```python
import jax
import jax.numpy as jnp
import numpy as np
from jax import lax
from jax.experimental import pallas as pl
from jax.experimental.pallas import tpu as pltpu
from jax.sharding import PartitionSpec as P


LEAF = 128
RANK = 32
RHS = 32
LPD = 64
NEAR = 9
FAR = 27
LOCAL = LPD * NEAR - 256
UNROLL = 8
UP_UNROLL = 4
WINDOW = 2176
LIST = 640
AXES = ("leaf", "sub")
MIB = 1024 * 1024
RATE = float(-4.0 / np.log(2.0))
TINY = 1e-30
f32 = jnp.float32
bf16 = jnp.bfloat16
VMEM = pl.BlockSpec(memory_space=pltpu.VMEM)
SMEM = pl.BlockSpec(memory_space=pltpu.SMEM)
HBM = pl.BlockSpec(memory_space=pltpu.HBM)


def decay(delta_x, delta_y):
    square = jnp.maximum(delta_x * delta_x + delta_y * delta_y, TINY)
    return jnp.exp2((square * lax.rsqrt(square)) * RATE)


def split(x):
    high = x.astype(bf16)
    return high, (x - high.astype(f32)).astype(bf16)


def dot(a, b, contract=((1,), (0,))):
    return lax.dot_general(a, b, (contract, ((), ())), preferred_element_type=f32)


def dot3(a, b, contract=((1,), (0,))):
    a_high, a_low = split(a)
    b_high, b_low = split(b)
    return (
        dot(a_high, b_high, contract) + dot(a_high, b_low, contract) + dot(a_low, b_high, contract)
    )


def lanes(x, lane):
    index = jnp.full(x.shape, lane, jnp.int32)
    return jnp.take_along_axis(x, index, axis=1, mode="promise_in_bounds")


def fetch(pairs, semaphores):
    copies = [
        pltpu.make_async_copy(source, target, semaphores.at[number])
        for number, (source, target) in enumerate(pairs)
    ]
    for copy in copies:
        copy.start()
    return copies


def pack_kernel(order_in, points_in, values_in, out, order, points, values, semaphores):
    pairs = ((order_in, order), (points_in, points), (values_in, values))
    for copy in fetch(pairs, semaphores):
        copy.wait()
    for leaf in range(LPD):
        columns = pl.ds(pl.multiple_of(order[leaf] * LEAF, LEAF), LEAF)
        out[32 * leaf : 32 * leaf + 32, :] = values[:, columns]
        out[2048 + 2 * leaf : 2048 + 2 * leaf + 2, :] = points[:, columns]


def up_kernel(
    device,
    near_in,
    pack,
    basis_in,
    low_in,
    top_in,
    proxy_in,
    halo,
    weights_out,
    tasks,
    near,
    basis,
    low,
    top,
    proxy,
    weights,
    coef,
    semaphores,
):
    pairs = (
        (near_in, near),
        (low_in, low),
        (basis_in, basis),
        (top_in, top),
        (proxy_in, proxy),
    )
    copies = fetch(pairs, semaphores)
    base = device[0] * LPD
    row_block = lax.broadcasted_iota(jnp.int32, (128, 128), 0) // 32
    lane_block = lax.broadcasted_iota(jnp.int32, (128, 128), 1) // 32
    diagonal = row_block == lane_block
    for copy in copies[:3]:
        copy.wait()

    def sort_leaf(leaf, local):
        code = leaf * 4096 + 1024 - base
        for k in range(NEAR):
            entry = near[k, leaf]
            offset = entry - base
            home = (offset >= 0) & (offset < LPD)
            where = jnp.where(home, local, (leaf * NEAR + (k + LOCAL)) - local)
            tasks[where] = entry + code
            local = local + home.astype(jnp.int32)
        return local

    def cluster(number, local):
        transfer = low[number]
        stacked = jnp.where(diagonal, jnp.concatenate([transfer] * 4, axis=0), 0.0)
        bases = basis[pl.ds(4 * number, 4)].reshape(128, LEAF)
        product = dot3(stacked, bases)
        rows = pl.ds(pl.multiple_of(128 * number, 128), 128)
        weights[rows, :] = product
        x = pack[rows, :]
        wide_w = jnp.concatenate([product[32 * m : 32 * m + 32] for m in range(4)], axis=1)
        wide_x = jnp.concatenate([x[32 * m : 32 * m + 32] for m in range(4)], axis=1)
        coef[pl.ds(pl.multiple_of(32 * number, 32), 32), 0:32] = dot3(
            wide_w, wide_x, ((1,), (1,))
        )
        for m in range(4):
            local = sort_leaf(4 * number + m, local)
        return local

    lax.fori_loop(0, 16, cluster, jnp.int32(0), unroll=UP_UNROLL)
    save = pltpu.make_async_copy(weights, weights_out, semaphores.at[5])
    save.start()
    for copy in copies[3:]:
        copy.wait()
    coefs = coef[:, 0:32]
    for block in range(4):
        halo[0:128, 32 * block : 32 * block + 32] = coefs[128 * block : 128 * block + 128]
    partial = dot3(top[...].reshape(512, 32), coefs, ((0,), (0,)))
    for block in range(4):
        halo[128:136, 32 * block : 32 * block + 32] = partial[8 * block : 8 * block + 8]
    for block in range(4):
        for i in range(4):
            halo[136 + 2 * block : 138 + 2 * block, 32 * i : 32 * i + 32] = proxy[4 * block + i]
    save.wait()


def near_loop(tasks, begin, count, place, columns, table, acc, spread, blocks):
    def decode(trip, u):
        index = trip * UNROLL + u
        task = tasks[begin + jnp.clip(index, 0, count - 1)]
        leaf = jnp.where((index >= 0) & (index < count), task >> 12, LPD)
        return leaf, task >> 12, place((task >> 6) & 63), task & (LPD - 1)

    def widen(trip):
        for u in range(UNROLL):
            _, _, slot, source = decode(trip, u)
            points = columns[pl.ds(pl.multiple_of(slot * 128, 128), 128), :]
            spread[u, 0:128, :] = lanes(points, 2 * source)
            spread[u, 128:256, :] = lanes(points, 2 * source + 1)

    def make(trip, target):
        for u in range(UNROLL):
            _, leaf, _, _ = decode(trip, u)
            row_x = target[pl.ds(2048 + 2 * leaf, 1), :]
            row_y = target[pl.ds(2049 + 2 * leaf, 1), :]
            kernel = decay(spread[u, 0:128, :] - row_x, spread[u, 128:256, :] - row_y)
            high, low = split(kernel)
            blocks[u, 0:128, :] = high
            blocks[u, 128:256, :] = low

    def multiply(trip):
        for u in range(UNROLL):
            leaf, _, slot, source = decode(trip, u)
            at = pl.multiple_of(slot * 2048 + 32 * source, 32)
            high, low = split(table[pl.ds(at, 32), :])
            left = jnp.concatenate(
                [
                    jnp.concatenate([high, high], axis=1),
                    jnp.concatenate([low, jnp.zeros_like(low)], axis=1),
                ],
                axis=0,
            )
            result = dot(left, blocks[u])
            rows = pl.ds(pl.multiple_of(32 * leaf, 32), 32)
            acc[rows, :] += result[0:32] + result[32:64]

    return widen, make, multiply


def near_run(count, widen, make, multiply, target):
    def step(trip, carry):
        multiply(trip - 2)
        make(trip - 1, target)
        widen(trip)
        return carry

    lax.fori_loop(0, count // UNROLL + 2, step, 0)


def local_kernel(begin, count, *refs):
    tasks, pack = refs[:2]
    before = refs[2] if begin else None
    out, acc, spread, blocks, columns = refs[-5:]
    acc[0:2048, :] = before[...] if begin else jnp.zeros((2048, 128), f32)
    columns[...] = pack[2048:2176, :].T
    parts = near_loop(
        tasks, begin, count, lambda code: 0, columns, pack, acc, spread, blocks
    )
    near_run(count, *parts, pack)
    out[...] = acc[0:2048, :]


def remote_kernel(begin, count, tasks, pack, north, west, east, south, before, *refs):
    out, acc, spread, blocks, columns, table, slots = refs
    for number, (fetched, code) in enumerate(((north, 0), (west, 15), (east, 17), (south, 32))):
        slots[code] = number
        columns[128 * number : 128 * number + 128, :] = fetched[2048:2176, :].T
        table[2048 * number : 2048 * number + 2048, :] = fetched[0:2048, :]
    acc[0:2048, :] = before[...]
    parts = near_loop(
        tasks, begin, count, lambda code: slots[code], columns, table, acc, spread, blocks
    )
    near_run(count, *parts, pack)
    out[...] = acc[0:2048, :]


def far_kernel(device, far, left, own, right, out):
    me = device[0]
    sources = [left[...], own[...], right[...]]
    stacked = jnp.concatenate(
        [h[0:128, 32 * g : 32 * g + 32] for h in sources for g in range(4)], axis=0
    )
    high, low = split(stacked)
    both = jnp.concatenate([high, low], axis=1)
    targets = own[136:144, :].T
    cluster_of = (
        lax.broadcasted_iota(jnp.int32, (16, 128), 0) * 4
        + lax.broadcasted_iota(jnp.int32, (16, 128), 1) // 32
    )
    for c in range(16):
        counts = jnp.zeros((16, 128), f32)
        for k in range(FAR):
            counts = counts + jnp.where(cluster_of == far[c, k] - (me - 1) * 16, 1.0, 0.0)
        rows = targets[32 * (c % 4) : 32 * (c % 4) + 32]
        lane = 2 * (c // 4)
        t_x = jnp.broadcast_to(rows[:, lane : lane + 1], (32, 128))
        t_y = jnp.broadcast_to(rows[:, lane + 1 : lane + 2], (32, 128))
        pieces = []
        for d in range(3):
            for g in range(4):
                s = sources[d][136 + 2 * g : 138 + 2 * g]
                pieces.append(
                    decay(t_x - s[0:1], t_y - s[1:2]) * counts[4 * d + g : 4 * d + g + 1]
                )
        kernel = jnp.concatenate(pieces, axis=1)
        k_high, k_low = split(kernel)
        first = dot(k_high, both)
        out[32 * c : 32 * c + 32, :] = first[:, 0:32] + first[:, 32:64] + dot(k_low, high)


def down_kernel(
    device, order, top_list, chip_map, piece_0, piece_1, piece_2, piece_3, proxy_top, top, low_part, weights, near, out, gathered, turned
):
    for number, piece in enumerate((piece_0, piece_1, piece_2, piece_3)):
        gathered[32 * number : 32 * number + 32] = piece[...]
    turned[...] = proxy_top[...].reshape(64, 128).T
    chip = device[0] // 2
    own_x, own_y, own_z = chip // 32, (chip // 8) % 4, chip % 8
    t_x = lanes(proxy_top[0], chip)
    t_y = lanes(proxy_top[1], chip)
    kernels = []
    rights = []
    for j in range(7):
        coordinates = []
        for i in range(4):
            k = min(4 * j + i, FAR - 1)
            source = chip_map[top_list[0, k]]
            coordinates.append(turned[pl.ds(source, 1), :])
            away_x = (own_x - source // 32 + 4) % 4
            away_y = (own_y - (source // 8) % 4 + 4) % 4
            away_z = (own_z - source % 8 + 8) % 8
            slot = (away_x * 4 + away_y) * 8 + away_z
            block = gathered[pl.ds(slot, 1)].reshape(8, 128)
            for g in range(4):
                rights.append(block[:, 32 * g : 32 * g + 32])
        s_x = jnp.concatenate([row[:, 0:32] for row in coordinates], axis=1)
        s_y = jnp.concatenate([row[:, 32:64] for row in coordinates], axis=1)
        kernel = decay(t_x - s_x, t_y - s_y)
        if 4 * j + 4 > FAR:
            used = lax.broadcasted_iota(jnp.int32, (32, 128), 1) < 32 * (FAR - 4 * j)
            kernel = jnp.where(used, kernel, 0.0)
        kernels.append(kernel)
    down_top = dot3(jnp.concatenate(kernels, axis=1), jnp.concatenate(rights, axis=0))
    down_low = low_part[...] + dot3(top[...].reshape(512, 32), down_top)
    for c in range(16):
        left = down_low[32 * c : 32 * c + 32].T
        right = jnp.concatenate(
            [weights[128 * c + 32 * m : 128 * c + 32 * m + 32, :] for m in range(4)], axis=1
        )
        result = dot3(left, right)
        for m in range(4):
            b = 4 * c + m
            columns = pl.ds(pl.multiple_of(order[b] * LEAF, LEAF), LEAF)
            out[:, columns] = result[:, 128 * m : 128 * m + 128] + near[32 * b : 32 * b + 32, :]


def call(body, out_shape, in_specs, out_specs, flops, mib, scratch=(), aliases=None):
    return pl.pallas_call(
        body,
        out_shape=out_shape,
        in_specs=in_specs,
        out_specs=out_specs,
        scratch_shapes=list(scratch),
        input_output_aliases=aliases or {},
        compiler_params=pltpu.CompilerParams(vmem_limit_bytes=mib * MIB),
        cost_estimate=pl.CostEstimate(flops=flops, bytes_accessed=0, transcendentals=0),
    )


def shape(*dims, dtype=f32):
    return jax.ShapeDtypeStruct(dims, dtype)


def device_shift(x, by, same_row):
    count = 256
    pairs = [
        (i, i + by)
        for i in range(count)
        if 0 <= i + by < count and (not same_row or i // 16 == (i + by) // 16)
    ]
    return lax.ppermute(x, AXES, pairs)


def chip_shift(x, by, size, stride):
    pairs = []
    for i in range(128):
        at = (i // stride) % size
        pairs.append((i, i + ((at + by) % size - at) * stride))
    return lax.ppermute(x, "leaf", pairs)


LOCAL_PARTS = (112, 104, 104)
REMOTE_PARTS = (128, 128)
MICRO = 2000000


def product(
    points,
    right_sides,
    leaf_order,
    leaf_basis,
    transfer_low,
    transfer_top,
    proxy_low,
    proxy_top,
    near_lists,
    far_lists,
    top_lists,
    subtree_map,
):
    device = lax.axis_index("leaf") * 2 + lax.axis_index("sub")
    device = device.astype(jnp.int32).reshape(1)
    pack = call(
        pack_kernel,
        shape(WINDOW, 128),
        [HBM, HBM, HBM],
        VMEM,
        2 * MICRO,
        62,
        [
            pltpu.SMEM((LPD,), jnp.int32),
            pltpu.VMEM((2, LPD * LEAF), f32),
            pltpu.VMEM((RHS, LPD * LEAF), f32),
            pltpu.SemaphoreType.DMA((3,)),
        ],
    )(leaf_order, points, right_sides)
    up = device_shift(pack, 16, False)
    down = device_shift(pack, -16, False)
    right = device_shift(pack, 1, True)
    left = device_shift(pack, -1, True)

    halo, weights, tasks = call(
        up_kernel,
        (shape(144, 128), shape(2048, 128), shape(LIST, dtype=jnp.int32)),
        [SMEM, HBM, VMEM, HBM, HBM, HBM, HBM],
        (VMEM, HBM, SMEM),
        4 * MICRO,
        62,
        [
            pltpu.SMEM((NEAR, LPD), jnp.int32),
            pltpu.VMEM((LPD, RANK, LEAF), f32),
            pltpu.VMEM((16, RANK, 128), f32),
            pltpu.VMEM((16, RANK, RANK), f32),
            pltpu.VMEM((16, 2, RANK), f32),
            pltpu.VMEM((2048, 128), f32),
            pltpu.VMEM((512, 128), f32),
            pltpu.SemaphoreType.DMA((6,)),
        ],
    )(device, near_lists.T, pack, leaf_basis, transfer_low, transfer_top, proxy_low)
    halo_left = device_shift(halo, 1, False)
    halo_right = device_shift(halo, -1, False)

    scratch = [
        pltpu.VMEM((2080, 128), f32),
        pltpu.VMEM((UNROLL, 256, 128), f32),
        pltpu.VMEM((UNROLL, 256, 128), bf16),
    ]
    near = None
    begin = 0
    for count in LOCAL_PARTS:

        def body(*refs, begin=begin, count=count):
            local_kernel(begin, count, *refs)

        operands = (tasks, pack) + ((near,) if begin else ())
        begin += count
        near = call(
            body,
            shape(2048, 128),
            [SMEM] + [VMEM] * (len(operands) - 1),
            VMEM,
            3 * MICRO,
            12,
            scratch + [pltpu.VMEM((128, 128), f32)],
        )(*operands)

    low_part = call(
        far_kernel, shape(512, 32), [SMEM, SMEM, VMEM, VMEM, VMEM], VMEM, 4 * MICRO, 12
    )(device, far_lists, halo_left, halo, halo_right)

    sibling = jnp.where(lax.axis_index("sub") == 0, halo_right[128:136], halo_left[128:136])
    gathered = (halo[128:136] + sibling).reshape(1, 8, 128)
    for number in range(3):
        other = chip_shift(gathered, 1 << number, 8, 1)
        gathered = jnp.concatenate([gathered, other], axis=0)
    pieces = [gathered]
    for by in range(1, 4):
        pieces.append(chip_shift(gathered, by, 4, 8))
    gathered = jnp.concatenate(pieces, axis=0)
    pieces = [gathered]
    for by in range(1, 4):
        pieces.append(chip_shift(gathered, by, 4, 32))

    for count in REMOTE_PARTS:

        def body(*refs, begin=begin, count=count):
            remote_kernel(begin, count, *refs)

        begin += count
        near = call(
            body,
            shape(2048, 128),
            [SMEM] + [VMEM] * 6,
            VMEM,
            4 * MICRO,
            24,
            scratch
            + [
                pltpu.VMEM((512, 128), f32),
                pltpu.VMEM((8192, 128), f32),
                pltpu.SMEM((64,), jnp.int32),
            ],
        )(tasks, pack, up, right, left, down, near)

    return call(
        down_kernel,
        shape(RHS, LPD * LEAF),
        [SMEM] * 4 + [VMEM] * 9,
        VMEM,
        4 * MICRO,
        20,
        [pltpu.VMEM((128, 8, 128), f32), pltpu.VMEM((128, 64), f32)],
    )(
        device,
        leaf_order,
        top_lists,
        subtree_map,
        *pieces,
        proxy_top.transpose(1, 2, 0),
        transfer_top,
        low_part,
        weights,
        near,
    )


def solution(mesh):
    return jax.shard_map(
        product,
        mesh=mesh,
        in_specs=(
            P(None, ("leaf", "sub")),
            P(None, ("leaf", "sub")),
            P(("leaf", "sub")),
            P(("leaf", "sub"), None, None),
            P(("leaf", "sub"), None, None),
            P(("leaf", "sub"), None, None),
            P(("leaf", "sub"), None, None),
            P(),
            P(("leaf", "sub"), None),
            P(("leaf", "sub"), None),
            P("leaf", None),
            P(),
        ),
        out_specs=P(None, ("leaf", "sub")),
        check_vma=False,
    )
```

```python
import jax
import jax.numpy as jnp
import numpy as np
from jax import lax
from jax.experimental import pallas as pl
from jax.experimental.pallas import tpu as pltpu
from jax.sharding import PartitionSpec as P


LEAF = 128
RANK = 32
RHS = 32
LPD = 64
NEAR = 9
FAR = 27
LOCAL = LPD * NEAR - 256
UNROLL = 8
UP_UNROLL = 4
HALO_AT = 2176
BUNDLE = HALO_AT + 144
LIST = 640
AXES = ("leaf", "sub")
MIB = 1024 * 1024
RATE = float(-4.0 / np.log(2.0))
TINY = 1e-30
f32 = jnp.float32
bf16 = jnp.bfloat16
VMEM = pl.BlockSpec(memory_space=pltpu.VMEM)
SMEM = pl.BlockSpec(memory_space=pltpu.SMEM)
HBM = pl.BlockSpec(memory_space=pltpu.HBM)


def decay(delta_x, delta_y):
    square = jnp.maximum(delta_x * delta_x + delta_y * delta_y, TINY)
    return jnp.exp2((square * lax.rsqrt(square)) * RATE)


def split(x):
    high = x.astype(bf16)
    return high, (x - high.astype(f32)).astype(bf16)


def dot(a, b, contract=((1,), (0,))):
    return lax.dot_general(a, b, (contract, ((), ())), preferred_element_type=f32)


def dot3(a, b, contract=((1,), (0,))):
    a_high, a_low = split(a)
    b_high, b_low = split(b)
    return (
        dot(a_high, b_high, contract) + dot(a_high, b_low, contract) + dot(a_low, b_high, contract)
    )


def lanes(x, lane):
    index = jnp.full(x.shape, lane, jnp.int32)
    return jnp.take_along_axis(x, index, axis=1, mode="promise_in_bounds")


def fetch(pairs, semaphores):
    copies = [
        pltpu.make_async_copy(source, target, semaphores.at[number])
        for number, (source, target) in enumerate(pairs)
    ]
    for copy in copies:
        copy.start()
    return copies


def up_kernel(
    device,
    order_in,
    near_in,
    points_in,
    values_in,
    basis_in,
    low_in,
    top_in,
    proxy_in,
    bundle_out,
    weights_out,
    tasks,
    order,
    near,
    points,
    values,
    basis,
    low,
    top,
    proxy,
    weights,
    bundle,
    coef,
    semaphores,
):
    pairs = (
        (order_in, order),
        (near_in, near),
        (values_in, values),
        (points_in, points),
        (low_in, low),
        (basis_in, basis),
        (top_in, top),
        (proxy_in, proxy),
    )
    copies = fetch(pairs, semaphores)
    halo = bundle.at[pl.ds(HALO_AT, 144)]
    base = device[0] * LPD
    row_block = lax.broadcasted_iota(jnp.int32, (128, 128), 0) // 32
    lane_block = lax.broadcasted_iota(jnp.int32, (128, 128), 1) // 32
    diagonal = row_block == lane_block
    for copy in copies[:4]:
        copy.wait()
    for leaf in range(LPD):
        block = pl.ds(pl.multiple_of(order[leaf] * LEAF, LEAF), LEAF)
        bundle[32 * leaf : 32 * leaf + 32, :] = values[:, block]
        bundle[2048 + 2 * leaf : 2048 + 2 * leaf + 2, :] = points[:, block]

    def publish(at, rows, number):
        part = pl.ds(at, rows)
        return pltpu.make_async_copy(
            bundle.at[part], bundle_out.at[part], semaphores.at[12 + number]
        )

    publish(0, HALO_AT, 0).start()
    for copy in copies[4:6]:
        copy.wait()

    def save(part):
        rows = pl.ds(512 * part, 512)
        return pltpu.make_async_copy(
            weights.at[rows], weights_out.at[rows], semaphores.at[8 + part]
        )

    def sort_leaf(leaf, local):
        code = leaf * 4096 + 1024 - base
        for k in range(NEAR):
            entry = near[k, leaf]
            home = (entry >> 6) == device[0]
            where = jnp.where(home, local, (leaf * NEAR + (k + LOCAL)) - local)
            tasks[where] = entry + code
            local = local + home.astype(jnp.int32)
        return local

    def cluster(number, local):
        transfer = low[number]
        stacked = jnp.where(diagonal, jnp.concatenate([transfer] * 4, axis=0), 0.0)
        bases = basis[pl.ds(4 * number, 4)].reshape(128, LEAF)
        product = dot3(stacked, bases)
        rows = pl.ds(pl.multiple_of(128 * number, 128), 128)
        weights[rows, :] = product
        x = bundle[rows, :]
        wide_w = jnp.concatenate([product[32 * m : 32 * m + 32] for m in range(4)], axis=1)
        wide_x = jnp.concatenate([x[32 * m : 32 * m + 32] for m in range(4)], axis=1)
        coef[pl.ds(pl.multiple_of(32 * number, 32), 32), 0:32] = dot3(
            wide_w, wide_x, ((1,), (1,))
        )
        for m in range(4):
            local = sort_leaf(4 * number + m, local)
        return local

    local = jnp.int32(0)
    for part in range(4):
        local = lax.fori_loop(4 * part, 4 * part + 4, cluster, local, unroll=UP_UNROLL)
        save(part).start()
    for copy in copies[6:]:
        copy.wait()
    coefs = coef[:, 0:32]
    for block in range(4):
        halo[0:128, 32 * block : 32 * block + 32] = coefs[128 * block : 128 * block + 128]
    partial = dot3(top[...].reshape(512, 32), coefs, ((0,), (0,)))
    for block in range(4):
        halo[128:136, 32 * block : 32 * block + 32] = partial[8 * block : 8 * block + 8]
    for block in range(4):
        for i in range(4):
            halo[136 + 2 * block : 138 + 2 * block, 32 * i : 32 * i + 32] = proxy[4 * block + i]
    publish(HALO_AT, 144, 1).start()
    publish(0, HALO_AT, 0).wait()
    for part in range(4):
        save(part).wait()
    publish(HALO_AT, 144, 1).wait()


def near_run(tasks, begin, count, place, columns, table, target, acc, spread, blocks):
    def decode(trip, u):
        index = trip * UNROLL + u
        task = tasks[begin + jnp.clip(index, 0, count - 1)]
        leaf = jnp.where((index >= 0) & (index < count), task >> 12, LPD)
        return leaf, task >> 12, place((task >> 6) & 63), task & (LPD - 1)

    def widen(trip, u):
        _, _, slot, source = decode(trip, u)
        points = columns[pl.ds(pl.multiple_of(slot * 128, 128), 128), :]
        spread[u, 0:128, :] = lanes(points, 2 * source)
        spread[u, 128:256, :] = lanes(points, 2 * source + 1)

    def make(trip, u):
        _, leaf, _, _ = decode(trip, u)
        row_x = target[pl.ds(2048 + 2 * leaf, 1), :]
        row_y = target[pl.ds(2049 + 2 * leaf, 1), :]
        kernel = decay(spread[u, 0:128, :] - row_x, spread[u, 128:256, :] - row_y)
        high, low = split(kernel)
        blocks[u, 0:128, :] = high
        blocks[u, 128:256, :] = low

    def multiply(trip, u):
        leaf, _, slot, source = decode(trip, u)
        at = pl.multiple_of(slot * 2048 + 32 * source, 32)
        high, low = split(table[pl.ds(at, 32), :])
        left = jnp.concatenate(
            [
                jnp.concatenate([high, high], axis=1),
                jnp.concatenate([low, jnp.zeros_like(low)], axis=1),
            ],
            axis=0,
        )
        result = dot(left, blocks[u])
        rows = pl.ds(pl.multiple_of(32 * leaf, 32), 32)
        acc[rows, :] += result[0:32] + result[32:64]

    def step(trip, carry):
        for u in range(UNROLL):
            multiply(trip - 2, u)
            make(trip - 1, u)
            widen(trip, u)
        return carry

    lax.fori_loop(0, count // UNROLL + 2, step, 0)


def local_kernel(begin, count, *refs):
    tasks_in, pack = refs[:2]
    before = refs[2] if begin else None
    out, acc, spread, blocks, tasks, columns, semaphores = refs[-7:]
    (copy,) = fetch([(tasks_in, tasks)], semaphores)
    acc[0:2048, :] = before[...] if begin else jnp.zeros((2048, 128), f32)
    columns[...] = pack[2048:2176, :].T
    copy.wait()
    near_run(tasks, begin, count, lambda code: 0, columns, pack, pack, acc, spread, blocks)
    out[...] = acc[0:2048, :]


def remote_kernel(begin, count, device, tasks_in, pack, near_0, near_1, near_2, near_3, before, *refs):
    out, acc, spread, blocks, tasks, columns, table, points, slots, semaphores = refs
    fetched = (near_0, near_1, near_2, near_3)
    pairs = [(tasks_in, tasks)]
    for number in range(4):
        pairs.append((fetched[number].at[pl.ds(2048, 128)], points.at[pl.ds(128 * number, 128)]))
        pairs.append((fetched[number].at[pl.ds(0, 2048)], table.at[pl.ds(2048 * number, 2048)]))
    copies = fetch(pairs, semaphores)
    acc[0:2048, :] = before[...]
    row, column = (device[0] >> 4) & 1, device[0] & 1
    slots[0], slots[32] = 1 - row, row
    slots[15], slots[17] = 3 - column, 2 + column
    copies[0].wait()
    for number in range(4):
        copies[2 * number + 1].wait()
        columns[128 * number : 128 * number + 128, :] = points[
            128 * number : 128 * number + 128, :
        ].T
    for number in range(4):
        copies[2 * number + 2].wait()
    near_run(
        tasks, begin, count, lambda code: slots[code], columns, table, pack, acc, spread, blocks
    )
    out[...] = acc[0:2048, :]


def far_kernel(device, far_in, beside_in, own_in, across_in, out, far, halos, semaphores):
    me = device[0]
    pairs = [(far_in, far)]
    for number, bundle in enumerate((beside_in, own_in, across_in)):
        pairs.append((bundle.at[pl.ds(HALO_AT, 144)], halos.at[number]))
    for copy in fetch(pairs, semaphores):
        copy.wait()
    sources = [halos[0], halos[1], halos[2]]
    step = 16 - 32 * (me & 1)
    stacked = jnp.concatenate(
        [h[0:128, 32 * g : 32 * g + 32] for h in sources for g in range(4)], axis=0
    )
    high, low = split(stacked)
    both = jnp.concatenate([high, low], axis=1)
    targets = halos[1, 136:144, :].T
    row = lax.broadcasted_iota(jnp.int32, (16, 128), 0)
    side = 1 - jnp.minimum(row >> 2, 2)
    cluster_of = (
        me * 16 + side * step + (row & 3) * 4 + (lax.broadcasted_iota(jnp.int32, (16, 128), 1) >> 5)
    )
    for c in range(16):
        counts = jnp.zeros((16, 128), f32)
        for k in range(FAR):
            counts = counts + jnp.where(cluster_of == far[c, k], 1.0, 0.0)
        rows = targets[32 * (c % 4) : 32 * (c % 4) + 32]
        lane = 2 * (c // 4)
        t_x = jnp.broadcast_to(rows[:, lane : lane + 1], (32, 128))
        t_y = jnp.broadcast_to(rows[:, lane + 1 : lane + 2], (32, 128))
        pieces = []
        for d in range(3):
            for g in range(4):
                s = sources[d][136 + 2 * g : 138 + 2 * g]
                pieces.append(
                    decay(t_x - s[0:1], t_y - s[1:2]) * counts[4 * d + g : 4 * d + g + 1]
                )
        kernel = jnp.concatenate(pieces, axis=1)
        k_high, k_low = split(kernel)
        first = dot(k_high, both)
        out[32 * c : 32 * c + 32, :] = first[:, 0:32] + first[:, 32:64] + dot(k_low, high)


def down_kernel(
    device, order, top_list, chip_map, piece_0, piece_1, piece_2, piece_3, proxy_top, top, low_part, weights, near, out, gathered, turned
):
    for number, piece in enumerate((piece_0, piece_1, piece_2, piece_3)):
        gathered[32 * number : 32 * number + 32] = piece[...]
    turned[...] = proxy_top[...].reshape(64, 128).T
    chip = device[0] // 2
    t_x = lanes(proxy_top[0], chip)
    t_y = lanes(proxy_top[1], chip)
    kernels = []
    rights = []
    for j in range(7):
        coordinates = []
        for i in range(4):
            k = min(4 * j + i, FAR - 1)
            source = chip_map[top_list[0, k]]
            coordinates.append(turned[pl.ds(source, 1), :])
            slot = chip ^ source
            block = gathered[pl.ds(slot, 1)].reshape(8, 128)
            for g in range(4):
                rights.append(block[:, 32 * g : 32 * g + 32])
        s_x = jnp.concatenate([row[:, 0:32] for row in coordinates], axis=1)
        s_y = jnp.concatenate([row[:, 32:64] for row in coordinates], axis=1)
        kernel = decay(t_x - s_x, t_y - s_y)
        if 4 * j + 4 > FAR:
            used = lax.broadcasted_iota(jnp.int32, (32, 128), 1) < 32 * (FAR - 4 * j)
            kernel = jnp.where(used, kernel, 0.0)
        kernels.append(kernel)
    down_top = dot3(jnp.concatenate(kernels, axis=1), jnp.concatenate(rights, axis=0))
    down_low = low_part[...] + dot3(top[...].reshape(512, 32), down_top)
    for c in range(16):
        left = down_low[32 * c : 32 * c + 32].T
        right = jnp.concatenate(
            [weights[128 * c + 32 * m : 128 * c + 32 * m + 32, :] for m in range(4)], axis=1
        )
        result = dot3(left, right)
        for m in range(4):
            b = 4 * c + m
            columns = pl.ds(pl.multiple_of(order[b] * LEAF, LEAF), LEAF)
            out[:, columns] = result[:, 128 * m : 128 * m + 128] + near[32 * b : 32 * b + 32, :]


def call(body, out_shape, in_specs, out_specs, flops, mib, scratch=(), aliases=None):
    return pl.pallas_call(
        body,
        out_shape=out_shape,
        in_specs=in_specs,
        out_specs=out_specs,
        scratch_shapes=list(scratch),
        input_output_aliases=aliases or {},
        compiler_params=pltpu.CompilerParams(vmem_limit_bytes=mib * MIB),
        cost_estimate=pl.CostEstimate(flops=flops, bytes_accessed=0, transcendentals=0),
    )


def shape(*dims, dtype=f32):
    return jax.ShapeDtypeStruct(dims, dtype)


def swap(x, first, by, row):
    pairs = []
    for i in range(256):
        other = i + by
        if (i // by) % 2 == first and other < 256 and i // row == other // row:
            pairs += [(i, other), (other, i)]
    return lax.ppermute(x, AXES, pairs)


def chip_swap(x, bits):
    return lax.ppermute(x, "leaf", [(i, i ^ bits) for i in range(128)])


LOCAL_PARTS = (112, 104, 104)
REMOTE_PARTS = (256,)
MICRO = 2000000


def product(
    points,
    right_sides,
    leaf_order,
    leaf_basis,
    transfer_low,
    transfer_top,
    proxy_low,
    proxy_top,
    near_lists,
    far_lists,
    top_lists,
    subtree_map,
):
    device = lax.axis_index("leaf") * 2 + lax.axis_index("sub")
    device = device.astype(jnp.int32).reshape(1)
    pack, weights, tasks = call(
        up_kernel,
        (shape(BUNDLE, 128), shape(2048, 128), shape(LIST, dtype=jnp.int32)),
        [SMEM] + [HBM] * 8,
        (HBM, HBM, SMEM),
        4 * MICRO,
        62,
        [
            pltpu.SMEM((LPD,), jnp.int32),
            pltpu.SMEM((NEAR, LPD), jnp.int32),
            pltpu.VMEM((2, LPD * LEAF), f32),
            pltpu.VMEM((RHS, LPD * LEAF), f32),
            pltpu.VMEM((LPD, RANK, LEAF), f32),
            pltpu.VMEM((16, RANK, 128), f32),
            pltpu.VMEM((16, RANK, RANK), f32),
            pltpu.VMEM((16, 2, RANK), f32),
            pltpu.VMEM((2048, 128), f32),
            pltpu.VMEM((BUNDLE, 128), f32),
            pltpu.VMEM((512, 128), f32),
            pltpu.SemaphoreType.DMA((14,)),
        ],
    )(
        device,
        leaf_order,
        near_lists.T,
        points,
        right_sides,
        leaf_basis,
        transfer_low,
        transfer_top,
        proxy_low,
    )
    near_2 = swap(pack, 0, 1, 256)
    near_3 = swap(pack, 1, 1, 256)
    near_0 = swap(pack, 0, 16, 256)
    near_1 = swap(pack, 1, 16, 256)

    scratch = [
        pltpu.VMEM((2080, 128), f32),
        pltpu.VMEM((UNROLL, 256, 128), f32),
        pltpu.VMEM((UNROLL, 256, 128), bf16),
        pltpu.SMEM((LIST,), jnp.int32),
    ]
    near = None
    begin = 0
    for count in LOCAL_PARTS:

        def body(*refs, begin=begin, count=count):
            local_kernel(begin, count, *refs)

        operands = (tasks, pack) + ((near,) if begin else ())
        begin += count
        near = call(
            body,
            shape(2048, 128),
            [HBM] + [VMEM] * (len(operands) - 1),
            VMEM,
            3 * MICRO,
            12,
            scratch + [pltpu.VMEM((128, 128), f32), pltpu.SemaphoreType.DMA((1,))],
        )(*operands)

    low_part = call(
        far_kernel,
        shape(512, 32),
        [SMEM] + [HBM] * 4,
        VMEM,
        4 * MICRO,
        12,
        [
            pltpu.SMEM((16, FAR), jnp.int32),
            pltpu.VMEM((3, 144, 128), f32),
            pltpu.SemaphoreType.DMA((4,)),
        ],
    )(device, far_lists, near_2, pack, near_3)

    partials = slice(HALO_AT + 128, HALO_AT + 136)
    gathered = (pack[partials] + near_2[partials]).reshape(1, 8, 128)
    for number in range(3):
        other = chip_swap(gathered, 1 << number)
        gathered = jnp.concatenate([gathered, other], axis=0)
    pieces = [gathered]
    for by in range(1, 4):
        pieces.append(chip_swap(gathered, 8 * by))
    gathered = jnp.concatenate(pieces, axis=0)
    pieces = [gathered]
    for by in range(1, 4):
        pieces.append(chip_swap(gathered, 32 * by))

    for count in REMOTE_PARTS:

        def body(*refs, begin=begin, count=count):
            remote_kernel(begin, count, *refs)

        begin += count
        near = call(
            body,
            shape(2048, 128),
            [SMEM, HBM, VMEM, HBM, HBM, HBM, HBM, VMEM],
            VMEM,
            4 * MICRO,
            24,
            scratch
            + [
                pltpu.VMEM((512, 128), f32),
                pltpu.VMEM((8192, 128), f32),
                pltpu.VMEM((512, 128), f32),
                pltpu.SMEM((64,), jnp.int32),
                pltpu.SemaphoreType.DMA((9,)),
            ],
        )(device, tasks, pack, near_0, near_1, near_2, near_3, near)

    return call(
        down_kernel,
        shape(RHS, LPD * LEAF),
        [SMEM] * 4 + [VMEM] * 9,
        VMEM,
        4 * MICRO,
        20,
        [pltpu.VMEM((128, 8, 128), f32), pltpu.VMEM((128, 64), f32)],
    )(
        device,
        leaf_order,
        top_lists,
        subtree_map,
        *pieces,
        proxy_top.transpose(1, 2, 0),
        transfer_top,
        low_part,
        weights,
        near,
    )


def solution(mesh):
    return jax.shard_map(
        product,
        mesh=mesh,
        in_specs=(
            P(None, ("leaf", "sub")),
            P(None, ("leaf", "sub")),
            P(("leaf", "sub")),
            P(("leaf", "sub"), None, None),
            P(("leaf", "sub"), None, None),
            P(("leaf", "sub"), None, None),
            P(("leaf", "sub"), None, None),
            P(),
            P(("leaf", "sub"), None),
            P(("leaf", "sub"), None),
            P("leaf", None),
            P(),
        ),
        out_specs=P(None, ("leaf", "sub")),
        check_vma=False,
    )
```

```python
import jax
import jax.numpy as jnp
import numpy as np
from jax import lax
from jax.experimental import pallas as pl
from jax.experimental.pallas import tpu as pltpu
from jax.sharding import PartitionSpec as P


LEAF = 128
RANK = 32
RHS = 32
LPD = 64
NEAR = 9
FAR = 27
LOCAL = LPD * NEAR - 256
NEAR_UNROLL = 8
FAR_UNROLL = 16
UP_UNROLL = 4
HALO_AT = 2176
BUNDLE = HALO_AT + 144
LIST = 640
AXES = ("leaf", "sub")
MIB = 1024 * 1024
RATE = float(-4.0 / np.log(2.0))
TINY = 1e-30
f32 = jnp.float32
bf16 = jnp.bfloat16
VMEM = pl.BlockSpec(memory_space=pltpu.VMEM)
SMEM = pl.BlockSpec(memory_space=pltpu.SMEM)
HBM = pl.BlockSpec(memory_space=pltpu.HBM)


def decay(delta_x, delta_y):
    square = jnp.maximum(delta_x * delta_x + delta_y * delta_y, TINY)
    return jnp.exp2((square * lax.rsqrt(square)) * RATE)


def split(x):
    high = x.astype(bf16)
    return high, (x - high.astype(f32)).astype(bf16)


def dot(a, b, contract=((1,), (0,))):
    return lax.dot_general(a, b, (contract, ((), ())), preferred_element_type=f32)


def dot3(a, b, contract=((1,), (0,))):
    a_high, a_low = split(a)
    b_high, b_low = split(b)
    return (
        dot(a_high, b_high, contract) + dot(a_high, b_low, contract) + dot(a_low, b_high, contract)
    )


def lanes(x, lane):
    index = jnp.full(x.shape, lane, jnp.int32)
    return jnp.take_along_axis(x, index, axis=1, mode="promise_in_bounds")


def fetch(pairs, semaphores):
    copies = [
        pltpu.make_async_copy(source, target, semaphores.at[number])
        for number, (source, target) in enumerate(pairs)
    ]
    for copy in copies:
        copy.start()
    return copies


def up_kernel(
    device,
    order_in,
    near_in,
    points_in,
    values_in,
    basis_in,
    low_in,
    top_in,
    proxy_in,
    bundle_out,
    weights_out,
    tasks,
    order,
    near,
    points,
    values,
    basis,
    low,
    top,
    proxy,
    weights,
    bundle,
    coef,
    semaphores,
):
    pairs = (
        (order_in, order),
        (near_in, near),
        (values_in, values),
        (points_in, points),
        (low_in, low),
        (basis_in, basis),
        (top_in, top),
        (proxy_in, proxy),
    )
    copies = fetch(pairs, semaphores)
    halo = bundle.at[pl.ds(HALO_AT, 144)]
    base = device[0] * LPD
    row_block = lax.broadcasted_iota(jnp.int32, (128, 128), 0) // 32
    lane_block = lax.broadcasted_iota(jnp.int32, (128, 128), 1) // 32
    diagonal = row_block == lane_block
    for copy in copies[:4]:
        copy.wait()
    for leaf in range(LPD):
        block = pl.ds(pl.multiple_of(order[leaf] * LEAF, LEAF), LEAF)
        bundle[32 * leaf : 32 * leaf + 32, :] = values[:, block]
        bundle[2048 + 2 * leaf : 2048 + 2 * leaf + 2, :] = points[:, block]

    def publish(at, rows, number):
        part = pl.ds(at, rows)
        return pltpu.make_async_copy(
            bundle.at[part], bundle_out.at[part], semaphores.at[12 + number]
        )

    publish(0, HALO_AT, 0).start()
    for copy in copies[4:6]:
        copy.wait()

    def save(part):
        rows = pl.ds(512 * part, 512)
        return pltpu.make_async_copy(
            weights.at[rows], weights_out.at[rows], semaphores.at[8 + part]
        )

    def sort_leaf(leaf, local):
        code = leaf * 4096 + 1024 - base
        for k in range(NEAR):
            entry = near[k, leaf]
            home = (entry >> 6) == device[0]
            where = jnp.where(home, local, (leaf * NEAR + (k + LOCAL)) - local)
            tasks[where] = entry + code
            local = local + home.astype(jnp.int32)
        return local

    def cluster(number, local):
        transfer = low[number]
        stacked = jnp.where(diagonal, jnp.concatenate([transfer] * 4, axis=0), 0.0)
        bases = basis[pl.ds(4 * number, 4)].reshape(128, LEAF)
        product = dot3(stacked, bases)
        rows = pl.ds(pl.multiple_of(128 * number, 128), 128)
        weights[rows, :] = product
        x = bundle[rows, :]
        wide_w = jnp.concatenate([product[32 * m : 32 * m + 32] for m in range(4)], axis=1)
        wide_x = jnp.concatenate([x[32 * m : 32 * m + 32] for m in range(4)], axis=1)
        coef[pl.ds(pl.multiple_of(32 * number, 32), 32), 0:32] = dot3(
            wide_w, wide_x, ((1,), (1,))
        )
        for m in range(4):
            local = sort_leaf(4 * number + m, local)
        return local

    local = jnp.int32(0)
    for part in range(4):
        local = lax.fori_loop(4 * part, 4 * part + 4, cluster, local, unroll=UP_UNROLL)
        save(part).start()
    for copy in copies[6:]:
        copy.wait()
    coefs = coef[:, 0:32]
    for block in range(4):
        halo[0:128, 32 * block : 32 * block + 32] = coefs[128 * block : 128 * block + 128]
    partial = dot3(top[...].reshape(512, 32), coefs, ((0,), (0,)))
    for block in range(4):
        halo[128:136, 32 * block : 32 * block + 32] = partial[8 * block : 8 * block + 8]
    for block in range(4):
        for i in range(4):
            halo[136 + 2 * block : 138 + 2 * block, 32 * i : 32 * i + 32] = proxy[4 * block + i]
    publish(HALO_AT, 144, 1).start()
    publish(0, HALO_AT, 0).wait()
    for part in range(4):
        save(part).wait()
    publish(HALO_AT, 144, 1).wait()


def near_run(tasks, begin, count, place, columns, table, target, acc, spread, blocks, ready=()):
    group = spread.shape[0]
    trips = count // group

    def decode(trip, u):
        task = tasks[begin + trip * group + u]
        return task >> 12, place((task >> 6) & 63), task & (LPD - 1)

    def widen(trip, u):
        _, slot, source = decode(trip, u)
        points = columns[pl.ds(pl.multiple_of(slot * 128, 128), 128), :]
        spread[u, 0:128, :] = lanes(points, 2 * source)
        spread[u, 128:256, :] = lanes(points, 2 * source + 1)

    def make(trip, u):
        leaf, _, _ = decode(trip, u)
        row_x = target[pl.ds(2048 + 2 * leaf, 1), :]
        row_y = target[pl.ds(2049 + 2 * leaf, 1), :]
        kernel = decay(spread[u, 0:128, :] - row_x, spread[u, 128:256, :] - row_y)
        high, low = split(kernel)
        blocks[u, 0:128, :] = high
        blocks[u, 128:256, :] = low

    def multiply(trip, u):
        leaf, slot, source = decode(trip, u)
        at = pl.multiple_of(slot * 2048 + 32 * source, 32)
        high, low = split(table[pl.ds(at, 32), :])
        left = jnp.concatenate(
            [
                jnp.concatenate([high, high], axis=1),
                jnp.concatenate([low, jnp.zeros_like(low)], axis=1),
            ],
            axis=0,
        )
        result = dot(left, blocks[u])
        rows = pl.ds(pl.multiple_of(32 * leaf, 32), 32)
        acc[rows, :] += result[0:32] + result[32:64]

    def step(trip, carry):
        for u in range(group):
            multiply(trip - 2, u)
        for u in range(group):
            make(trip - 1, u)
        for u in range(group):
            widen(trip, u)
        return carry

    for u in range(group):
        widen(0, u)
    for u in range(group):
        make(0, u)
    for u in range(group):
        widen(1, u)
    for copy in ready:
        copy.wait()
    lax.fori_loop(2, trips, step, 0)
    for u in range(group):
        multiply(trips - 2, u)
    for u in range(group):
        make(trips - 1, u)
    for u in range(group):
        multiply(trips - 1, u)


def local_kernel(begin, count, *refs):
    tasks_in, pack = refs[:2]
    before = refs[2] if begin else None
    out, acc, spread, blocks, tasks, columns, semaphores = refs[-7:]
    (copy,) = fetch([(tasks_in, tasks)], semaphores)
    acc[...] = before[...] if begin else jnp.zeros((2048, 128), f32)
    columns[...] = pack[2048:2176, :].T
    copy.wait()
    near_run(tasks, begin, count, lambda code: 0, columns, pack, pack, acc, spread, blocks)
    out[...] = acc[...]


def remote_kernel(begin, count, device, tasks_in, pack, near_0, near_1, near_2, near_3, before, *refs):
    out, acc, spread, blocks, tasks, columns, table, points, slots, semaphores = refs
    fetched = (near_0, near_1, near_2, near_3)
    pairs = [(tasks_in, tasks)]
    for number in range(4):
        pairs.append((fetched[number].at[pl.ds(2048, 128)], points.at[pl.ds(128 * number, 128)]))
        pairs.append((fetched[number].at[pl.ds(0, 2048)], table.at[pl.ds(2048 * number, 2048)]))
    copies = fetch(pairs, semaphores)
    acc[...] = before[...]
    row, column = (device[0] >> 4) & 1, device[0] & 1
    slots[0], slots[32] = 1 - row, row
    slots[15], slots[17] = 3 - column, 2 + column
    copies[0].wait()
    for number in range(4):
        copies[2 * number + 1].wait()
        columns[128 * number : 128 * number + 128, :] = points[
            128 * number : 128 * number + 128, :
        ].T
    near_run(
        tasks,
        begin,
        count,
        lambda code: slots[code],
        columns,
        table,
        pack,
        acc,
        spread,
        blocks,
        [copies[2 * number + 2] for number in range(4)],
    )
    out[...] = acc[...]


def far_kernel(device, far_in, beside_in, own_in, across_in, out, far, halos, semaphores):
    me = device[0]
    pairs = [(far_in, far)]
    for number, bundle in enumerate((beside_in, own_in, across_in)):
        pairs.append((bundle.at[pl.ds(HALO_AT, 144)], halos.at[number]))
    for copy in fetch(pairs, semaphores):
        copy.wait()
    sources = [halos[0], halos[1], halos[2]]
    step = 16 - 32 * (me & 1)
    stacked = jnp.concatenate(
        [h[0:128, 32 * g : 32 * g + 32] for h in sources for g in range(4)], axis=0
    )
    high, low = split(stacked)
    both = jnp.concatenate([high, low], axis=1)
    targets = halos[1, 136:144, :].T
    row = lax.broadcasted_iota(jnp.int32, (16, 128), 0)
    side = 1 - jnp.minimum(row >> 2, 2)
    cluster_of = (
        me * 16 + side * step + (row & 3) * 4 + (lax.broadcasted_iota(jnp.int32, (16, 128), 1) >> 5)
    )
    for c in range(16):
        counts = jnp.zeros((16, 128), f32)
        for k in range(FAR):
            counts = counts + jnp.where(cluster_of == far[c, k], 1.0, 0.0)
        rows = targets[32 * (c % 4) : 32 * (c % 4) + 32]
        lane = 2 * (c // 4)
        t_x = jnp.broadcast_to(rows[:, lane : lane + 1], (32, 128))
        t_y = jnp.broadcast_to(rows[:, lane + 1 : lane + 2], (32, 128))
        pieces = []
        for d in range(3):
            for g in range(4):
                s = sources[d][136 + 2 * g : 138 + 2 * g]
                pieces.append(
                    decay(t_x - s[0:1], t_y - s[1:2]) * counts[4 * d + g : 4 * d + g + 1]
                )
        kernel = jnp.concatenate(pieces, axis=1)
        k_high, k_low = split(kernel)
        first = dot(k_high, both)
        out[32 * c : 32 * c + 32, :] = first[:, 0:32] + first[:, 32:64] + dot(k_low, high)


def down_kernel(
    device, order_in, list_in, map_in, piece_0, piece_1, piece_2, piece_3, proxy_top, top, low_part, weights, near, out, gathered, turned, order, top_list, chip_map, semaphores
):
    copies = fetch(((list_in, top_list), (map_in, chip_map), (order_in, order)), semaphores)
    for number, piece in enumerate((piece_0, piece_1, piece_2, piece_3)):
        gathered[32 * number : 32 * number + 32] = piece[...]
    turned[...] = proxy_top[...].reshape(64, 128).T
    for copy in copies:
        copy.wait()
    chip = device[0] // 2
    t_x = lanes(proxy_top[0], chip)
    t_y = lanes(proxy_top[1], chip)
    kernels = []
    rights = []
    for j in range(7):
        coordinates = []
        for i in range(4):
            k = min(4 * j + i, FAR - 1)
            source = chip_map[top_list[0, k]]
            coordinates.append(turned[pl.ds(source, 1), :])
            slot = chip ^ source
            block = gathered[pl.ds(slot, 1)].reshape(8, 128)
            for g in range(4):
                rights.append(block[:, 32 * g : 32 * g + 32])
        s_x = jnp.concatenate([row[:, 0:32] for row in coordinates], axis=1)
        s_y = jnp.concatenate([row[:, 32:64] for row in coordinates], axis=1)
        kernel = decay(t_x - s_x, t_y - s_y)
        if 4 * j + 4 > FAR:
            used = lax.broadcasted_iota(jnp.int32, (32, 128), 1) < 32 * (FAR - 4 * j)
            kernel = jnp.where(used, kernel, 0.0)
        kernels.append(kernel)
    down_top = dot3(jnp.concatenate(kernels, axis=1), jnp.concatenate(rights, axis=0))
    down_low = low_part[...] + dot3(top[...].reshape(512, 32), down_top)
    for c in range(16):
        left = down_low[32 * c : 32 * c + 32].T
        right = jnp.concatenate(
            [weights[128 * c + 32 * m : 128 * c + 32 * m + 32, :] for m in range(4)], axis=1
        )
        result = dot3(left, right)
        for m in range(4):
            b = 4 * c + m
            columns = pl.ds(pl.multiple_of(order[b] * LEAF, LEAF), LEAF)
            out[:, columns] = result[:, 128 * m : 128 * m + 128] + near[32 * b : 32 * b + 32, :]


def call(body, out_shape, in_specs, out_specs, flops, mib, scratch=(), aliases=None):
    return pl.pallas_call(
        body,
        out_shape=out_shape,
        in_specs=in_specs,
        out_specs=out_specs,
        scratch_shapes=list(scratch),
        input_output_aliases=aliases or {},
        compiler_params=pltpu.CompilerParams(vmem_limit_bytes=mib * MIB),
        cost_estimate=pl.CostEstimate(flops=flops, bytes_accessed=0, transcendentals=0),
    )


def shape(*dims, dtype=f32):
    return jax.ShapeDtypeStruct(dims, dtype)


def swap(x, first, by, row):
    pairs = []
    for i in range(256):
        other = i + by
        if (i // by) % 2 == first and other < 256 and i // row == other // row:
            pairs += [(i, other), (other, i)]
    return lax.ppermute(x, AXES, pairs)


def chip_swap(x, bits):
    return lax.ppermute(x, "leaf", [(i, i ^ bits) for i in range(128)])


LOCAL_PARTS = (112, 104, 104)
REMOTE_PARTS = (256,)
MICRO = 2000000


def product(
    points,
    right_sides,
    leaf_order,
    leaf_basis,
    transfer_low,
    transfer_top,
    proxy_low,
    proxy_top,
    near_lists,
    far_lists,
    top_lists,
    subtree_map,
):
    device = lax.axis_index("leaf") * 2 + lax.axis_index("sub")
    device = device.astype(jnp.int32).reshape(1)
    pack, weights, tasks = call(
        up_kernel,
        (shape(BUNDLE, 128), shape(2048, 128), shape(LIST, dtype=jnp.int32)),
        [SMEM] + [HBM] * 8,
        (HBM, HBM, SMEM),
        4 * MICRO,
        62,
        [
            pltpu.SMEM((LPD,), jnp.int32),
            pltpu.SMEM((NEAR, LPD), jnp.int32),
            pltpu.VMEM((2, LPD * LEAF), f32),
            pltpu.VMEM((RHS, LPD * LEAF), f32),
            pltpu.VMEM((LPD, RANK, LEAF), f32),
            pltpu.VMEM((16, RANK, 128), f32),
            pltpu.VMEM((16, RANK, RANK), f32),
            pltpu.VMEM((16, 2, RANK), f32),
            pltpu.VMEM((2048, 128), f32),
            pltpu.VMEM((BUNDLE, 128), f32),
            pltpu.VMEM((512, 128), f32),
            pltpu.SemaphoreType.DMA((14,)),
        ],
    )(
        device,
        leaf_order,
        near_lists.T,
        points,
        right_sides,
        leaf_basis,
        transfer_low,
        transfer_top,
        proxy_low,
    )
    near_2 = swap(pack, 0, 1, 256)
    near_3 = swap(pack, 1, 1, 256)
    near_0 = swap(pack, 0, 16, 256)
    near_1 = swap(pack, 1, 16, 256)

    def scratch(group):
        return [
            pltpu.VMEM((2048, 128), f32),
            pltpu.VMEM((group, 256, 128), f32),
            pltpu.VMEM((group, 256, 128), bf16),
            pltpu.SMEM((LIST,), jnp.int32),
        ]

    near = None
    begin = 0
    for count in LOCAL_PARTS:

        def body(*refs, begin=begin, count=count):
            local_kernel(begin, count, *refs)

        operands = (tasks, pack) + ((near,) if begin else ())
        begin += count
        near = call(
            body,
            shape(2048, 128),
            [HBM] + [VMEM] * (len(operands) - 1),
            VMEM,
            3 * MICRO,
            12,
            scratch(NEAR_UNROLL) + [pltpu.VMEM((128, 128), f32), pltpu.SemaphoreType.DMA((1,))],
        )(*operands)

    low_part = call(
        far_kernel,
        shape(512, 32),
        [SMEM] + [HBM] * 4,
        VMEM,
        4 * MICRO,
        12,
        [
            pltpu.SMEM((16, FAR), jnp.int32),
            pltpu.VMEM((3, 144, 128), f32),
            pltpu.SemaphoreType.DMA((4,)),
        ],
    )(device, far_lists, near_2, pack, near_3)

    partials = slice(HALO_AT + 128, HALO_AT + 136)
    gathered = (pack[partials] + near_2[partials]).reshape(1, 8, 128)
    for number in range(3):
        other = chip_swap(gathered, 1 << number)
        gathered = jnp.concatenate([gathered, other], axis=0)
    pieces = [gathered]
    for by in range(1, 4):
        pieces.append(chip_swap(gathered, 8 * by))
    gathered = jnp.concatenate(pieces, axis=0)
    pieces = [gathered]
    for by in range(1, 4):
        pieces.append(chip_swap(gathered, 32 * by))

    for count in REMOTE_PARTS:

        def body(*refs, begin=begin, count=count):
            remote_kernel(begin, count, *refs)

        begin += count
        near = call(
            body,
            shape(2048, 128),
            [SMEM, HBM, VMEM, HBM, HBM, HBM, HBM, VMEM],
            VMEM,
            4 * MICRO,
            24,
            scratch(FAR_UNROLL)
            + [
                pltpu.VMEM((512, 128), f32),
                pltpu.VMEM((8192, 128), f32),
                pltpu.VMEM((512, 128), f32),
                pltpu.SMEM((64,), jnp.int32),
                pltpu.SemaphoreType.DMA((9,)),
            ],
        )(device, tasks, pack, near_0, near_1, near_2, near_3, near)

    return call(
        down_kernel,
        shape(RHS, LPD * LEAF),
        [SMEM] + [HBM] * 3 + [VMEM] * 9,
        VMEM,
        4 * MICRO,
        20,
        [
            pltpu.VMEM((128, 8, 128), f32),
            pltpu.VMEM((128, 64), f32),
            pltpu.SMEM((LPD,), jnp.int32),
            pltpu.SMEM((1, FAR), jnp.int32),
            pltpu.SMEM((128,), jnp.int32),
            pltpu.SemaphoreType.DMA((3,)),
        ],
    )(
        device,
        leaf_order,
        top_lists,
        subtree_map,
        *pieces,
        proxy_top.transpose(1, 2, 0),
        transfer_top,
        low_part,
        weights,
        near,
    )


def solution(mesh):
    return jax.shard_map(
        product,
        mesh=mesh,
        in_specs=(
            P(None, ("leaf", "sub")),
            P(None, ("leaf", "sub")),
            P(("leaf", "sub")),
            P(("leaf", "sub"), None, None),
            P(("leaf", "sub"), None, None),
            P(("leaf", "sub"), None, None),
            P(("leaf", "sub"), None, None),
            P(),
            P(("leaf", "sub"), None),
            P(("leaf", "sub"), None),
            P("leaf", None),
            P(),
        ),
        out_specs=P(None, ("leaf", "sub")),
        check_vma=False,
    )
```

```python
import jax
import jax.numpy as jnp
import numpy as np
from jax import lax
from jax.experimental import pallas as pl
from jax.experimental.pallas import tpu as pltpu
from jax.sharding import PartitionSpec as P


LEAF = 128
RANK = 32
RHS = 32
LPD = 64
NEAR = 9
FAR = 27
LOCAL = LPD * NEAR - 256
NEAR_UNROLL = 16
FAR_UNROLL = 16
UP_UNROLL = 4
HALO_AT = 2176
BUNDLE = HALO_AT + 144
LIST = 640
AXES = ("leaf", "sub")
MIB = 1024 * 1024
RATE = float(-4.0 / np.log(2.0))
TINY = 1e-30
f32 = jnp.float32
bf16 = jnp.bfloat16
VMEM = pl.BlockSpec(memory_space=pltpu.VMEM)
SMEM = pl.BlockSpec(memory_space=pltpu.SMEM)
HBM = pl.BlockSpec(memory_space=pltpu.HBM)


def decay(delta_x, delta_y):
    square = jnp.maximum(delta_x * delta_x + delta_y * delta_y, TINY)
    return jnp.exp2((square * lax.rsqrt(square)) * RATE)


def split(x):
    high = x.astype(bf16)
    return high, (x - high.astype(f32)).astype(bf16)


def dot(a, b, contract=((1,), (0,))):
    return lax.dot_general(a, b, (contract, ((), ())), preferred_element_type=f32)


def dot3(a, b, contract=((1,), (0,))):
    a_high, a_low = split(a)
    b_high, b_low = split(b)
    return (
        dot(a_high, b_high, contract) + dot(a_high, b_low, contract) + dot(a_low, b_high, contract)
    )


def lanes(x, lane):
    index = jnp.full(x.shape, lane, jnp.int32)
    return jnp.take_along_axis(x, index, axis=1, mode="promise_in_bounds")


def fetch(pairs, semaphores):
    copies = [
        pltpu.make_async_copy(source, target, semaphores.at[number])
        for number, (source, target) in enumerate(pairs)
    ]
    for copy in copies:
        copy.start()
    return copies


def up_kernel(
    device,
    order_in,
    near_in,
    points_in,
    values_in,
    basis_in,
    low_in,
    top_in,
    proxy_in,
    bundle_out,
    weights_out,
    tasks,
    order,
    near,
    points,
    values,
    basis,
    low,
    top,
    proxy,
    weights,
    bundle,
    coef,
    semaphores,
):
    pairs = (
        (order_in, order),
        (near_in, near),
        (values_in, values),
        (points_in, points),
        (low_in, low),
        (basis_in, basis),
        (top_in, top),
        (proxy_in, proxy),
    )
    copies = fetch(pairs, semaphores)
    halo = bundle.at[pl.ds(HALO_AT, 144)]
    base = device[0] * LPD
    row_block = lax.broadcasted_iota(jnp.int32, (128, 128), 0) // 32
    lane_block = lax.broadcasted_iota(jnp.int32, (128, 128), 1) // 32
    diagonal = row_block == lane_block
    for copy in copies[:4]:
        copy.wait()
    for leaf in range(LPD):
        block = pl.ds(pl.multiple_of(order[leaf] * LEAF, LEAF), LEAF)
        bundle[32 * leaf : 32 * leaf + 32, :] = values[:, block]
        bundle[2048 + 2 * leaf : 2048 + 2 * leaf + 2, :] = points[:, block]

    def publish(at, rows, number):
        part = pl.ds(at, rows)
        return pltpu.make_async_copy(
            bundle.at[part], bundle_out.at[part], semaphores.at[12 + number]
        )

    publish(0, HALO_AT, 0).start()
    for copy in copies[4:6]:
        copy.wait()

    def save(part):
        rows = pl.ds(512 * part, 512)
        return pltpu.make_async_copy(
            weights.at[rows], weights_out.at[rows], semaphores.at[8 + part]
        )

    def sort_leaf(leaf, local):
        code = leaf * 4096 + 1024 - base
        entries = [near[k, leaf] for k in range(NEAR)]
        for k, entry in enumerate(entries):
            home = (entry >> 6) == device[0]
            where = jnp.where(home, local, (leaf * NEAR + (k + LOCAL)) - local)
            tasks[where] = entry + code
            local = local + home.astype(jnp.int32)
        return local

    def cluster(number, local):
        transfer = low[number]
        stacked = jnp.where(diagonal, jnp.concatenate([transfer] * 4, axis=0), 0.0)
        bases = basis[pl.ds(4 * number, 4)].reshape(128, LEAF)
        product = dot3(stacked, bases)
        rows = pl.ds(pl.multiple_of(128 * number, 128), 128)
        weights[rows, :] = product
        x = bundle[rows, :]
        wide_w = jnp.concatenate([product[32 * m : 32 * m + 32] for m in range(4)], axis=1)
        wide_x = jnp.concatenate([x[32 * m : 32 * m + 32] for m in range(4)], axis=1)
        coef[pl.ds(pl.multiple_of(32 * number, 32), 32), 0:32] = dot3(
            wide_w, wide_x, ((1,), (1,))
        )
        for m in range(4):
            local = sort_leaf(4 * number + m, local)
        return local

    local = jnp.int32(0)
    for part in range(4):
        local = lax.fori_loop(4 * part, 4 * part + 4, cluster, local, unroll=UP_UNROLL)
        save(part).start()
    for copy in copies[6:]:
        copy.wait()
    coefs = coef[:, 0:32]
    for block in range(4):
        halo[0:128, 32 * block : 32 * block + 32] = coefs[128 * block : 128 * block + 128]
    partial = dot3(top[...].reshape(512, 32), coefs, ((0,), (0,)))
    for block in range(4):
        halo[128:136, 32 * block : 32 * block + 32] = partial[8 * block : 8 * block + 8]
    for block in range(4):
        for i in range(4):
            halo[136 + 2 * block : 138 + 2 * block, 32 * i : 32 * i + 32] = proxy[4 * block + i]
    publish(HALO_AT, 144, 1).start()
    publish(0, HALO_AT, 0).wait()
    for part in range(4):
        save(part).wait()
    publish(HALO_AT, 144, 1).wait()


def near_run(tasks, begin, count, place, columns, table, target, acc, spread, blocks, ready=()):
    group = spread.shape[0]
    trips = count // group

    def decode(trip, u):
        task = tasks[begin + trip * group + u]
        return task >> 12, place((task >> 6) & 63), task & (LPD - 1)

    def widen(trip, u):
        _, slot, source = decode(trip, u)
        points = columns[pl.ds(pl.multiple_of(slot * 128, 128), 128), :]
        spread[u, 0:128, :] = lanes(points, 2 * source)
        spread[u, 128:256, :] = lanes(points, 2 * source + 1)

    def make(trip, u):
        leaf, _, _ = decode(trip, u)
        row_x = target[pl.ds(2048 + 2 * leaf, 1), :]
        row_y = target[pl.ds(2049 + 2 * leaf, 1), :]
        kernel = decay(spread[u, 0:128, :] - row_x, spread[u, 128:256, :] - row_y)
        high, low = split(kernel)
        blocks[u, 0:128, :] = high
        blocks[u, 128:256, :] = low

    def multiply(trip, u):
        leaf, slot, source = decode(trip, u)
        at = pl.multiple_of(slot * 2048 + 32 * source, 32)
        high, low = split(table[pl.ds(at, 32), :])
        left = jnp.concatenate(
            [
                jnp.concatenate([high, high], axis=1),
                jnp.concatenate([low, jnp.zeros_like(low)], axis=1),
            ],
            axis=0,
        )
        result = dot(left, blocks[u])
        rows = pl.ds(pl.multiple_of(32 * leaf, 32), 32)
        acc[rows, :] += result[0:32] + result[32:64]

    def step(trip, carry):
        for u in range(group):
            multiply(trip - 2, u)
        for u in range(group):
            make(trip - 1, u)
        for u in range(group):
            widen(trip, u)
        return carry

    for u in range(group):
        widen(0, u)
    for u in range(group):
        make(0, u)
    for u in range(group):
        widen(1, u)
    for copy in ready:
        copy.wait()
    lax.fori_loop(2, trips, step, 0)
    for u in range(group):
        multiply(trips - 2, u)
    for u in range(group):
        make(trips - 1, u)
    for u in range(group):
        multiply(trips - 1, u)


def local_kernel(begin, count, *refs):
    tasks_in, pack = refs[:2]
    before = refs[2] if begin else None
    out, acc, spread, blocks, tasks, columns, semaphores = refs[-7:]
    (copy,) = fetch([(tasks_in, tasks)], semaphores)
    acc[...] = before[...] if begin else jnp.zeros((2048, 128), f32)
    columns[...] = pack[2048:2176, :].T
    copy.wait()
    near_run(tasks, begin, count, lambda code: 0, columns, pack, pack, acc, spread, blocks)
    out[...] = acc[...]


def remote_kernel(begin, count, device, tasks_in, pack, near_0, near_1, near_2, near_3, before, *refs):
    out, acc, spread, blocks, tasks, columns, table, points, slots, semaphores = refs
    fetched = (near_0, near_1, near_2, near_3)
    pairs = [(tasks_in, tasks)]
    for number in range(4):
        pairs.append((fetched[number].at[pl.ds(2048, 128)], points.at[pl.ds(128 * number, 128)]))
        pairs.append((fetched[number].at[pl.ds(0, 2048)], table.at[pl.ds(2048 * number, 2048)]))
    copies = fetch(pairs, semaphores)
    acc[...] = before[...]
    row, column = (device[0] >> 4) & 1, device[0] & 1
    slots[0], slots[32] = 1 - row, row
    slots[15], slots[17] = 3 - column, 2 + column
    copies[0].wait()
    for number in range(4):
        copies[2 * number + 1].wait()
        columns[128 * number : 128 * number + 128, :] = points[
            128 * number : 128 * number + 128, :
        ].T
    near_run(
        tasks,
        begin,
        count,
        lambda code: slots[code],
        columns,
        table,
        pack,
        acc,
        spread,
        blocks,
        [copies[2 * number + 2] for number in range(4)],
    )
    out[...] = acc[...]


def far_kernel(device, far_in, beside_in, own_in, across_in, out, far, halos, semaphores):
    me = device[0]
    pairs = [(far_in, far)]
    for number, bundle in enumerate((beside_in, own_in, across_in)):
        pairs.append((bundle.at[pl.ds(HALO_AT, 144)], halos.at[number]))
    for copy in fetch(pairs, semaphores):
        copy.wait()
    sources = [halos[0], halos[1], halos[2]]
    step = 16 - 32 * (me & 1)
    stacked = jnp.concatenate(
        [h[0:128, 32 * g : 32 * g + 32] for h in sources for g in range(4)], axis=0
    )
    high, low = split(stacked)
    both = jnp.concatenate([high, low], axis=1)
    targets = halos[1, 136:144, :].T
    row = lax.broadcasted_iota(jnp.int32, (16, 128), 0)
    side = 1 - jnp.minimum(row >> 2, 2)
    cluster_of = (
        me * 16 + side * step + (row & 3) * 4 + (lax.broadcasted_iota(jnp.int32, (16, 128), 1) >> 5)
    )
    for c in range(16):
        counts = jnp.zeros((16, 128), f32)
        for k in range(FAR):
            counts = counts + jnp.where(cluster_of == far[c, k], 1.0, 0.0)
        rows = targets[32 * (c % 4) : 32 * (c % 4) + 32]
        lane = 2 * (c // 4)
        t_x = jnp.broadcast_to(rows[:, lane : lane + 1], (32, 128))
        t_y = jnp.broadcast_to(rows[:, lane + 1 : lane + 2], (32, 128))
        pieces = []
        for d in range(3):
            for g in range(4):
                s = sources[d][136 + 2 * g : 138 + 2 * g]
                pieces.append(
                    decay(t_x - s[0:1], t_y - s[1:2]) * counts[4 * d + g : 4 * d + g + 1]
                )
        kernel = jnp.concatenate(pieces, axis=1)
        k_high, k_low = split(kernel)
        first = dot(k_high, both)
        out[32 * c : 32 * c + 32, :] = first[:, 0:32] + first[:, 32:64] + dot(k_low, high)


def down_kernel(
    device, order_in, list_in, map_in, piece_0, piece_1, piece_2, piece_3, proxy_top, top, low_part, weights, near, out, gathered, turned, order, top_list, chip_map, semaphores
):
    copies = fetch(((list_in, top_list), (map_in, chip_map), (order_in, order)), semaphores)
    for number, piece in enumerate((piece_0, piece_1, piece_2, piece_3)):
        gathered[32 * number : 32 * number + 32] = piece[...]
    turned[...] = proxy_top[...].reshape(64, 128).T
    for copy in copies:
        copy.wait()
    chip = device[0] // 2
    t_x = lanes(proxy_top[0], chip)
    t_y = lanes(proxy_top[1], chip)
    kernels = []
    rights = []
    for j in range(7):
        coordinates = []
        for i in range(4):
            k = min(4 * j + i, FAR - 1)
            source = chip_map[top_list[0, k]]
            coordinates.append(turned[pl.ds(source, 1), :])
            slot = chip ^ source
            block = gathered[pl.ds(slot, 1)].reshape(8, 128)
            for g in range(4):
                rights.append(block[:, 32 * g : 32 * g + 32])
        s_x = jnp.concatenate([row[:, 0:32] for row in coordinates], axis=1)
        s_y = jnp.concatenate([row[:, 32:64] for row in coordinates], axis=1)
        kernel = decay(t_x - s_x, t_y - s_y)
        if 4 * j + 4 > FAR:
            used = lax.broadcasted_iota(jnp.int32, (32, 128), 1) < 32 * (FAR - 4 * j)
            kernel = jnp.where(used, kernel, 0.0)
        kernels.append(kernel)
    down_top = dot3(jnp.concatenate(kernels, axis=1), jnp.concatenate(rights, axis=0))
    down_low = low_part[...] + dot3(top[...].reshape(512, 32), down_top)
    for c in range(16):
        left = down_low[32 * c : 32 * c + 32].T
        right = jnp.concatenate(
            [weights[128 * c + 32 * m : 128 * c + 32 * m + 32, :] for m in range(4)], axis=1
        )
        result = dot3(left, right)
        for m in range(4):
            b = 4 * c + m
            columns = pl.ds(pl.multiple_of(order[b] * LEAF, LEAF), LEAF)
            out[:, columns] = result[:, 128 * m : 128 * m + 128] + near[32 * b : 32 * b + 32, :]


def call(body, out_shape, in_specs, out_specs, flops, mib, scratch=(), aliases=None):
    return pl.pallas_call(
        body,
        out_shape=out_shape,
        in_specs=in_specs,
        out_specs=out_specs,
        scratch_shapes=list(scratch),
        input_output_aliases=aliases or {},
        compiler_params=pltpu.CompilerParams(vmem_limit_bytes=mib * MIB),
        cost_estimate=pl.CostEstimate(flops=flops, bytes_accessed=0, transcendentals=0),
    )


def shape(*dims, dtype=f32):
    return jax.ShapeDtypeStruct(dims, dtype)


def swap(x, first, by, row):
    pairs = []
    for i in range(256):
        other = i + by
        if (i // by) % 2 == first and other < 256 and i // row == other // row:
            pairs += [(i, other), (other, i)]
    return lax.ppermute(x, AXES, pairs)


def chip_swap(x, bits):
    return lax.ppermute(x, "leaf", [(i, i ^ bits) for i in range(128)])


LOCAL_PARTS = (112, 112, 96)
REMOTE_PARTS = (256,)
MICRO = 2000000


def product(
    points,
    right_sides,
    leaf_order,
    leaf_basis,
    transfer_low,
    transfer_top,
    proxy_low,
    proxy_top,
    near_lists,
    far_lists,
    top_lists,
    subtree_map,
):
    device = lax.axis_index("leaf") * 2 + lax.axis_index("sub")
    device = device.astype(jnp.int32).reshape(1)
    pack, weights, tasks = call(
        up_kernel,
        (shape(BUNDLE, 128), shape(2048, 128), shape(LIST, dtype=jnp.int32)),
        [SMEM] + [HBM] * 8,
        (HBM, HBM, SMEM),
        4 * MICRO,
        62,
        [
            pltpu.SMEM((LPD,), jnp.int32),
            pltpu.SMEM((NEAR, LPD), jnp.int32),
            pltpu.VMEM((2, LPD * LEAF), f32),
            pltpu.VMEM((RHS, LPD * LEAF), f32),
            pltpu.VMEM((LPD, RANK, LEAF), f32),
            pltpu.VMEM((16, RANK, 128), f32),
            pltpu.VMEM((16, RANK, RANK), f32),
            pltpu.VMEM((16, 2, RANK), f32),
            pltpu.VMEM((2048, 128), f32),
            pltpu.VMEM((BUNDLE, 128), f32),
            pltpu.VMEM((512, 128), f32),
            pltpu.SemaphoreType.DMA((14,)),
        ],
    )(
        device,
        leaf_order,
        near_lists.T,
        points,
        right_sides,
        leaf_basis,
        transfer_low,
        transfer_top,
        proxy_low,
    )
    near_2 = swap(pack, 0, 1, 256)
    near_3 = swap(pack, 1, 1, 256)
    near_0 = swap(pack, 0, 16, 256)
    near_1 = swap(pack, 1, 16, 256)

    def scratch(group):
        return [
            pltpu.VMEM((2048, 128), f32),
            pltpu.VMEM((group, 256, 128), f32),
            pltpu.VMEM((group, 256, 128), bf16),
            pltpu.SMEM((LIST,), jnp.int32),
        ]

    near = None
    begin = 0
    for count in LOCAL_PARTS:

        def body(*refs, begin=begin, count=count):
            local_kernel(begin, count, *refs)

        operands = (tasks, pack) + ((near,) if begin else ())
        begin += count
        near = call(
            body,
            shape(2048, 128),
            [HBM] + [VMEM] * (len(operands) - 1),
            VMEM,
            3 * MICRO,
            12,
            scratch(NEAR_UNROLL) + [pltpu.VMEM((128, 128), f32), pltpu.SemaphoreType.DMA((1,))],
        )(*operands)

    low_part = call(
        far_kernel,
        shape(512, 32),
        [SMEM] + [HBM] * 4,
        VMEM,
        4 * MICRO,
        12,
        [
            pltpu.SMEM((16, FAR), jnp.int32),
            pltpu.VMEM((3, 144, 128), f32),
            pltpu.SemaphoreType.DMA((4,)),
        ],
    )(device, far_lists, near_2, pack, near_3)

    partials = slice(HALO_AT + 128, HALO_AT + 136)
    gathered = (pack[partials] + near_2[partials]).reshape(1, 8, 128)
    for number in range(3):
        other = chip_swap(gathered, 1 << number)
        gathered = jnp.concatenate([gathered, other], axis=0)
    pieces = [gathered]
    for by in range(1, 4):
        pieces.append(chip_swap(gathered, 8 * by))
    gathered = jnp.concatenate(pieces, axis=0)
    pieces = [gathered]
    for by in range(1, 4):
        pieces.append(chip_swap(gathered, 32 * by))

    for count in REMOTE_PARTS:

        def body(*refs, begin=begin, count=count):
            remote_kernel(begin, count, *refs)

        begin += count
        near = call(
            body,
            shape(2048, 128),
            [SMEM, HBM, VMEM, HBM, HBM, HBM, HBM, VMEM],
            VMEM,
            4 * MICRO,
            24,
            scratch(FAR_UNROLL)
            + [
                pltpu.VMEM((512, 128), f32),
                pltpu.VMEM((8192, 128), f32),
                pltpu.VMEM((512, 128), f32),
                pltpu.SMEM((64,), jnp.int32),
                pltpu.SemaphoreType.DMA((9,)),
            ],
        )(device, tasks, pack, near_0, near_1, near_2, near_3, near)

    return call(
        down_kernel,
        shape(RHS, LPD * LEAF),
        [SMEM] + [HBM] * 3 + [VMEM] * 9,
        VMEM,
        4 * MICRO,
        20,
        [
            pltpu.VMEM((128, 8, 128), f32),
            pltpu.VMEM((128, 64), f32),
            pltpu.SMEM((LPD,), jnp.int32),
            pltpu.SMEM((1, FAR), jnp.int32),
            pltpu.SMEM((128,), jnp.int32),
            pltpu.SemaphoreType.DMA((3,)),
        ],
    )(
        device,
        leaf_order,
        top_lists,
        subtree_map,
        *pieces,
        proxy_top.transpose(1, 2, 0),
        transfer_top,
        low_part,
        weights,
        near,
    )


def solution(mesh):
    return jax.shard_map(
        product,
        mesh=mesh,
        in_specs=(
            P(None, ("leaf", "sub")),
            P(None, ("leaf", "sub")),
            P(("leaf", "sub")),
            P(("leaf", "sub"), None, None),
            P(("leaf", "sub"), None, None),
            P(("leaf", "sub"), None, None),
            P(("leaf", "sub"), None, None),
            P(),
            P(("leaf", "sub"), None),
            P(("leaf", "sub"), None),
            P("leaf", None),
            P(),
        ),
        out_specs=P(None, ("leaf", "sub")),
        check_vma=False,
    )
```
